32 devices in a mesh: pipe: 2 (over core), dp: 8 (over z, y), tensor: 2 (over x).
Axes of the slice: x: 2, y: 2, z: 4, core: 2. Of those that a mesh axis runs over, the one named last changes fastest.
Arguments:
- hidden_in: bfloat16 [2, 16, 2, 64, 3584], P('pipe', 'dp'), may hold values from -60 to 60, as said below
- attention_probs: bfloat16 [2, 16, 2, 14, 64, 64], P('pipe', 'dp', None, 'tensor'), may hold values from 0 to 1, as said below
- norm_gain: float32 [2, 3584], P('pipe'), may hold values from 0.5 to 1.5
- value_weight: bfloat16 [2, 3584, 256], P('pipe', None, 'tensor'), may hold values from -0.09375 to 0.09375
- output_weight: bfloat16 [2, 1792, 3584], P('pipe', 'tensor'), may hold values from -0.125 to 0.125
- head_grad: bfloat16 [16, 2, 64, 3584], P('dp', 'tensor'), may hold values from -16 to 16
- policy_logprob: float32 [16, 2, 64], P('dp'), may hold values from -3 to -0.2
- reference_logprob: float32 [16, 2], P('dp'), may hold values from -96 to -12.8
- sequence_bounds: int32 [16, 3], P('dp'), may hold values from 1 to 64, as said below
Outputs:
- section_cotangent: bfloat16 [2, 16, 2, 64, 3584], P('pipe', 'dp', 'tensor')
- value_gradient: float32 [2, 3584, 256], P('pipe', 'dp', 'tensor')
- output_gradient: float32 [2, 3584, 1792], P('pipe', 'dp', 'tensor')
- gain_gradient: float32 [2, 3584], P('pipe', 'dp')
The draws below stay inside these ranges and needn't reach their ends.
Inputs may be any that keep to these rules, and one draw needn't show every extreme that they name: `sequence_bounds`: entry 0 is the prompt length, shared by the two sequences of a pair; a sequence's response is the positions from entry 0 up to its end (entry 1 for the chosen, entry 2 for the rejected sequence), and holds one position or more. `attention_probs`: each row is a causal attention distribution: zero above the diagonal, summing to one before rounding. `hidden_in`: activations of varying size from token to token.
All inputs are finite; a program needn't handle non-finite values.
Results may differ from the reference program's by a relative error of at most 0.017.
Values may be sent and summed in bfloat16 or wider, within the bound.
A program may use at most 128 MiB of HBM per device.

```python
import math
import jax
import jax.numpy as jnp
from jax import lax

D = 3584
HEADS = 14
KV_HEADS = 2
HEAD_DIM = 128
SEQ = 64
PAIRS = 16
N_PIPE = 2
N_TENSOR = 2


def draw_hidden_in(key, part):
    key_main, key_scale = jax.random.split(key, 2)
    full_shape = (N_PIPE, PAIRS, 2, SEQ, D)
    row_scale = jnp.exp(jax.random.uniform(key_scale, (N_PIPE, PAIRS, 2, SEQ, 1), jnp.float32, 0.0, math.log(10.0)))
    noise = jnp.clip(jax.random.normal(key_main, full_shape, jnp.float32), -6.0, 6.0)
    return (row_scale * noise).astype(jnp.bfloat16)


def draw_attention_probs(key, part):
    key_noise, key_temper, key_slope = jax.random.split(key, 3)
    full_shape = (N_PIPE, PAIRS, 2, HEADS, SEQ, SEQ)
    head_shape = (N_PIPE, 1, 1, HEADS, 1, 1)
    temper = jnp.exp(jax.random.uniform(key_temper, head_shape, jnp.float32, math.log(0.5), math.log(3.0)))
    decay_slope = jnp.exp(jax.random.uniform(key_slope, head_shape, jnp.float32, math.log(0.5 / SEQ), 0.0))
    query_pos = jnp.arange(SEQ)[:, None]
    key_pos = jnp.arange(SEQ)[None, :]
    distance = (query_pos - key_pos).astype(jnp.float32)
    logits = jax.random.normal(key_noise, full_shape, jnp.float32) * temper - decay_slope * distance
    logits = jnp.where(key_pos <= query_pos, logits, -1000000000.0)
    return jax.nn.softmax(logits, axis=-1).astype(jnp.bfloat16)


def draw_sequence_bounds(key, part):
    key_prompt, key_extra, key_pick = jax.random.split(key, 3)
    pair_index = jnp.arange(PAIRS, dtype=jnp.int32)
    prompt = jax.random.randint(key_prompt, (PAIRS,), 1, SEQ // 4 + 1, jnp.int32)
    base_length = SEQ // 8 + SEQ // 2 * pair_index // PAIRS
    extra = jax.random.randint(key_extra, (PAIRS, 2), 0, SEQ // 8 + 1, jnp.int32)
    ends = jnp.minimum(prompt[:, None] + base_length[:, None] + extra, SEQ)
    picked = jax.random.randint(key_pick, (), 0, PAIRS, jnp.int32)
    full_end = (pair_index == picked)[:, None] & (jnp.arange(2, dtype=jnp.int32)[None, :] == 1)
    ends = jnp.where(full_end, SEQ, ends)
    return jnp.concatenate([prompt[:, None], ends], axis=1).astype(jnp.int32)


def levels(stream_key, dims, shards, smallest, largest):
    def one(position, shards_of):
        steps = jax.random.uniform(jax.random.fold_in(jax.random.fold_in(stream_key, 6), position), (shards_of,), jnp.float32, smallest / len(shards), largest / len(shards))
        return jnp.repeat(jnp.exp(steps), dims[position] // shards_of).reshape((-1,) + (1,) * (len(dims) - position - 1))

    factor_of = one(*shards[0])
    for cut in shards[1:]:
        factor_of = factor_of * one(*cut)
    return factor_of


def gaussian(stream_key, dims, deviation, most, cuts=(), held_as=jnp.bfloat16):
    factor_of = levels(stream_key, dims, cuts, -0.22, 0.18) if cuts else 1.0
    drawn = jax.random.normal(stream_key, dims, jnp.float32) * deviation * factor_of
    return jnp.minimum(jnp.maximum(drawn, -most), most).astype(held_as)


def setup_inputs(seed: int = 0) -> dict:
    key_of = jax.random.split(jax.random.key(seed), 10)
    hidden_in = draw_hidden_in(jax.random.fold_in(key_of[9], 71), 0)
    attention_probs = draw_attention_probs(jax.random.fold_in(key_of[9], 71), 0)
    norm_gain = jnp.clip(1.0 + 0.1 * jax.random.normal(key_of[2], (N_PIPE, D), jnp.float32), 0.5, 1.5)
    value_weight = gaussian(key_of[3], (N_PIPE, D, KV_HEADS * HEAD_DIM), D ** -0.5, 0.09375, ((0, 2), (2, 2)))
    output_weight = gaussian(key_of[4], (N_PIPE, HEADS * HEAD_DIM, D), (HEADS * HEAD_DIM) ** -0.5, 0.125, ((0, 2), (1, 2)))
    head_grad = gaussian(key_of[5], (PAIRS, 2, SEQ, D), 4.0, 16.0, ((0, 8), (1, 2)))
    policy_logprob = jnp.clip(-3.0 + 2.8 * jax.random.uniform(key_of[6], (PAIRS, 2, SEQ), jnp.float32) ** levels(key_of[6], (PAIRS, 2, SEQ), ((0, 8),), -0.2, 0.2), -3.0, -0.2)
    reference_logprob = jnp.clip(-96.0 + 83.2 * jax.random.uniform(key_of[7], (PAIRS, 2), jnp.float32) ** levels(key_of[7], (PAIRS, 2), ((0, 8),), -0.2, 0.2), -96.0, -12.8)
    sequence_bounds = draw_sequence_bounds(jax.random.fold_in(key_of[9], 71), 0)
    return dict(hidden_in=hidden_in, attention_probs=attention_probs, norm_gain=norm_gain, value_weight=value_weight, output_weight=output_weight, head_grad=head_grad, policy_logprob=policy_logprob, reference_logprob=reference_logprob, sequence_bounds=sequence_bounds)


EPSILON = 1e-06
DPO_BETA = 0.25
LIKELIHOOD_COEF = 0.2

def section_backward(inputs, pattern, gain_vector, value_matrix, output_matrix, upstream):
    group_size = HEADS // KV_HEADS
    input_float = inputs.astype(jnp.float32)
    inverse_rms = lax.rsqrt(lax.optimization_barrier(jnp.mean(input_float * input_float, axis=-1, keepdims=True)) + EPSILON)
    normed = (input_float * inverse_rms * gain_vector).astype(jnp.bfloat16)
    values = jnp.einsum('pcsd,dk->pcsk', normed.astype(jnp.float32), value_matrix.astype(jnp.float32)).astype(jnp.bfloat16)
    grouped = pattern.astype(jnp.float32).reshape(PAIRS, 2, KV_HEADS, group_size, SEQ, SEQ)
    values_heads = values.astype(jnp.float32).reshape(PAIRS, 2, SEQ, KV_HEADS, HEAD_DIM)
    mixed = jnp.einsum('pckgst,pctke->pcskge', grouped, values_heads).astype(jnp.bfloat16)
    mixed = mixed.reshape(PAIRS, 2, SEQ, HEADS * HEAD_DIM)
    upstream_float = upstream.astype(jnp.float32)
    mixed_grad = jnp.einsum('pcsd,hd->pcsh', upstream_float, output_matrix.astype(jnp.float32)).astype(jnp.bfloat16)
    mixed_heads = mixed_grad.astype(jnp.float32).reshape(PAIRS, 2, SEQ, KV_HEADS, group_size, HEAD_DIM)
    values_grad = jnp.einsum('pckgst,pcskge->pctke', grouped, mixed_heads).astype(jnp.bfloat16)
    values_grad = values_grad.reshape(PAIRS, 2, SEQ, KV_HEADS * HEAD_DIM)
    group_columns = KV_HEADS * HEAD_DIM // N_TENSOR
    grad_groups = values_grad.astype(jnp.float32).reshape(PAIRS, 2, SEQ, N_TENSOR, group_columns)
    weight_groups = value_matrix.astype(jnp.float32).reshape(D, N_TENSOR, group_columns)
    normed_grad = jnp.zeros((PAIRS, 2, SEQ, D), jnp.float32)
    for group_index in range(N_TENSOR):
        group_term = jnp.einsum('pcsk,dk->pcsd', grad_groups[:, :, :, group_index, :], weight_groups[:, group_index, :])
        rounded = lax.optimization_barrier(group_term.astype(jnp.bfloat16))
        normed_grad = normed_grad + rounded.astype(jnp.float32)
    gain_total = lax.optimization_barrier(jnp.sum(normed_grad * input_float * inverse_rms, axis=(0, 1, 2)))
    scaled = normed_grad * gain_vector
    cubed = inverse_rms * inverse_rms * inverse_rms
    input_grad = inverse_rms * scaled - input_float * cubed * lax.optimization_barrier(jnp.mean(input_float * scaled, axis=-1, keepdims=True))
    new_rows = (upstream_float + input_grad).astype(jnp.bfloat16)
    mixed_total = jnp.einsum('pcsd,pcsh->dh', upstream_float, mixed.astype(jnp.float32))
    value_total = jnp.einsum('pcsd,pcsk->dk', normed.astype(jnp.float32), values_grad.astype(jnp.float32))
    return (new_rows, value_total, mixed_total, gain_total)

def reference(hidden_in, attention_probs, norm_gain, value_weight, output_weight, head_grad, policy_logprob, reference_logprob, sequence_bounds):
    positions = jnp.arange(SEQ, dtype=jnp.int32)
    response_bool = (positions[None, None, :] >= sequence_bounds[:, 0:1, None]) & (positions[None, None, :] < sequence_bounds[:, 1:3, None])
    response_mask = response_bool.astype(jnp.float32)
    sequence_logprob = lax.optimization_barrier(jnp.sum(response_mask * policy_logprob, axis=-1))
    margin = DPO_BETA * (sequence_logprob[:, 0] - reference_logprob[:, 0] - (sequence_logprob[:, 1] - reference_logprob[:, 1]))
    weight_pair = jax.nn.sigmoid(-margin)
    chosen_total = jnp.sum(response_bool[:, 0, :].astype(jnp.int32))
    likelihood_scale = LIKELIHOOD_COEF * jnp.asarray(PAIRS, jnp.float32) / chosen_total.astype(jnp.float32)
    chosen_weight = -DPO_BETA * weight_pair[:, None] * response_mask[:, 0] - likelihood_scale * response_mask[:, 0]
    rejected_weight = DPO_BETA * weight_pair[:, None] * response_mask[:, 1]
    token_weight = jnp.stack([chosen_weight, rejected_weight], axis=1)
    upstream = (token_weight[..., None] * head_grad.astype(jnp.float32)).astype(jnp.bfloat16)
    cotangents = []
    value_list = []
    output_list = []
    gain_list = []
    for section_index in range(N_PIPE - 1, -1, -1):
        upstream, value_total, mixed_total, gain_total = section_backward(hidden_in[section_index], attention_probs[section_index], norm_gain[section_index], value_weight[section_index], output_weight[section_index], upstream)
        cotangents.insert(0, upstream)
        value_list.insert(0, value_total)
        output_list.insert(0, mixed_total)
        gain_list.insert(0, gain_total)
    return (jnp.stack(cotangents), jnp.stack(value_list), jnp.stack(output_list), jnp.stack(gain_list))
```

```python
import functools

import jax
import jax.numpy as jnp
from jax import lax
from jax.experimental import pallas as pl
from jax.experimental.pallas import tpu as pltpu
from jax.sharding import PartitionSpec as P

HEAD_DIM = 128
MESH = pl.DeviceIdType.MESH

EPSILON = 1e-06
DPO_BETA = 0.25
LIKELIHOOD_COEF = 0.2


def greet(axis, n):
    me = lax.axis_index(axis)
    barrier = pltpu.get_barrier_semaphore()

    @pl.loop(1, n)
    def _(k):
        pl.semaphore_signal(
            barrier, inc=1, device_id={axis: lax.rem(me + k, n)}, device_id_type=MESH
        )

    pl.semaphore_wait(barrier, n - 1)
    return me


def count_kernel(axis, n, count_ref, total_ref, landed, send_sem, recv_sem):
    me = greet(axis, n)

    def copy(k):
        return pltpu.make_async_remote_copy(
            src_ref=count_ref,
            dst_ref=landed.at[k],
            send_sem=send_sem.at[k],
            recv_sem=recv_sem.at[k],
            device_id={axis: lax.rem(me + k, n)},
            device_id_type=MESH,
        )

    @pl.loop(1, n)
    def _(k):
        copy(k).start()

    total_ref[...] = count_ref[...]

    @pl.loop(1, n)
    def _(k):
        copy(k).wait()
        total_ref[...] += landed[k]


def count_over(axis, count):
    n = lax.axis_size(axis)
    if n == 1:
        return count
    spread = jnp.broadcast_to(count, (8, 128))
    total = pl.pallas_call(
        functools.partial(count_kernel, axis, n),
        out_shape=jax.ShapeDtypeStruct((8, 128), jnp.int32),
        in_specs=[pl.BlockSpec(memory_space=pltpu.VMEM)],
        out_specs=pl.BlockSpec(memory_space=pltpu.VMEM),
        scratch_shapes=[
            pltpu.VMEM((n, 8, 128), jnp.int32),
            pltpu.SemaphoreType.DMA((n,)),
            pltpu.SemaphoreType.DMA((n,)),
        ],
        compiler_params=pltpu.CompilerParams(collective_id=0, has_side_effects=True),
        name="count",
    )(spread)
    return total[0, 0]


def gradient_kernel(
    axis,
    n,
    mixed_ref,
    dy_ref,
    value_ref,
    gain_ref,
    out_ref,
    value_out_ref,
    gain_out_ref,
    mixed_in,
    dy_in,
    value_in,
    gain_in,
    send_sem,
    recv_sem,
):
    me = greet(axis, n)

    def copies(k):
        peer = lax.rem(me + k, n)
        pairs = (
            (dy_ref.at[peer], dy_in.at[k]),
            (mixed_ref, mixed_in.at[k]),
            (value_ref.at[peer], value_in.at[k]),
            (gain_ref.at[peer], gain_in.at[k]),
        )
        return [
            pltpu.make_async_remote_copy(
                src_ref=src,
                dst_ref=dst,
                send_sem=send_sem.at[i, k],
                recv_sem=recv_sem.at[i, k],
                device_id={axis: peer},
                device_id_type=MESH,
            )
            for i, (src, dst) in enumerate(pairs)
        ]

    @pl.loop(1, n)
    def _(k):
        for c in copies(k):
            c.start()

    out_ref[...] = jnp.dot(dy_ref[me], mixed_ref[...], preferred_element_type=jnp.float32)
    value_out_ref[...] = value_ref[me].astype(jnp.float32)
    gain_out_ref[...] = gain_ref[me]

    @pl.loop(1, n)
    def _(k):
        for c in copies(k):
            c.wait_recv()
        out_ref[...] += jnp.dot(dy_in[k], mixed_in[k], preferred_element_type=jnp.float32)
        value_out_ref[...] += value_in[k].astype(jnp.float32)
        gain_out_ref[...] += gain_in[k]

    @pl.loop(1, n)
    def _(k):
        for c in copies(k):
            c.wait_send()


def gradients(axis, mixed, dy, value_part, gain_part):
    n, rows, tokens = dy.shape
    columns, value_columns = mixed.shape[1], value_part.shape[2]
    vmem = pl.BlockSpec(memory_space=pltpu.VMEM)
    return pl.pallas_call(
        functools.partial(gradient_kernel, axis, n),
        out_shape=(
            jax.ShapeDtypeStruct((rows, columns), jnp.float32),
            jax.ShapeDtypeStruct((rows, value_columns), jnp.float32),
            jax.ShapeDtypeStruct((1, rows), jnp.float32),
        ),
        in_specs=[vmem] * 4,
        out_specs=(vmem,) * 3,
        scratch_shapes=[
            pltpu.VMEM((n, tokens, columns), jnp.bfloat16),
            pltpu.VMEM((n, rows, tokens), jnp.bfloat16),
            pltpu.VMEM((n, rows, value_columns), jnp.bfloat16),
            pltpu.VMEM((n, 1, rows), jnp.float32),
            pltpu.SemaphoreType.DMA((4, n)),
            pltpu.SemaphoreType.DMA((4, n)),
        ],
        compiler_params=pltpu.CompilerParams(
            collective_id=1, has_side_effects=True, vmem_limit_bytes=56 * 2**20
        ),
        name="gradients",
    )(mixed, dy, value_part, gain_part)


def others(block, axis):
    n = lax.axis_size(axis)
    return [lax.ppermute(block, axis, [(i, (i + k) % n) for i in range(n)]) for k in range(1, n)]


def gathered(block, axis, dim):
    n = lax.axis_size(axis)
    me = lax.axis_index(axis)
    blocks = [block] + others(block, axis)
    ordered = []
    for j in range(n):
        pick = blocks[0]
        for k in range(1, n):
            pick = jnp.where(lax.rem(me - j + n, n) == k, blocks[k], pick)
        ordered.append(pick)
    return jnp.concatenate(ordered, axis=dim)


def body(
    hidden_in,
    attention_probs,
    norm_gain,
    value_weight,
    output_weight,
    head_grad,
    policy_logprob,
    reference_logprob,
    sequence_bounds,
):
    section_count = lax.axis_size("pipe")
    section_index = lax.axis_index("pipe")
    tensor_index = lax.axis_index("tensor")
    dp_count = lax.axis_size("dp")
    micro_count, _, sequence_length, model_width = hidden_in.shape[1:]
    tokens = micro_count * 2 * sequence_length
    value_columns = value_weight.shape[2]
    value_heads = value_columns // HEAD_DIM
    local_heads = attention_probs.shape[3]
    group_size = local_heads // value_heads
    mixed_columns = output_weight.shape[1]
    own_rows = 2 // lax.axis_size("tensor")
    gain_vector = norm_gain[0]
    value_matrix = value_weight[0]
    output_matrix = output_weight[0]
    full_head_grad = gathered(head_grad, "tensor", 1)
    value_matrices = [value_matrix] + others(value_matrix, "tensor")
    pattern = attention_probs[0].reshape(
        micro_count * 2, value_heads, group_size, sequence_length, sequence_length
    )
    positions = jnp.arange(sequence_length, dtype=jnp.int32)
    response_bool = (positions[None, None, :] >= sequence_bounds[:, 0:1, None]) & (
        positions[None, None, :] < sequence_bounds[:, 1:3, None]
    )
    chosen_total = count_over("dp", jnp.sum(response_bool[:, 0, :].astype(jnp.int32)))
    response_mask = response_bool.astype(jnp.float32)
    sequence_logprob = jnp.sum(response_mask * policy_logprob, axis=-1)
    margin = DPO_BETA * (
        sequence_logprob[:, 0]
        - reference_logprob[:, 0]
        - (sequence_logprob[:, 1] - reference_logprob[:, 1])
    )
    weight_pair = jax.nn.sigmoid(-margin)
    pair_total = micro_count * dp_count
    likelihood_scale = (
        LIKELIHOOD_COEF * jnp.asarray(pair_total, jnp.float32) / chosen_total.astype(jnp.float32)
    )
    chosen_weight = (
        -DPO_BETA * weight_pair[:, None] * response_mask[:, 0]
        - likelihood_scale * response_mask[:, 0]
    )
    rejected_weight = DPO_BETA * weight_pair[:, None] * response_mask[:, 1]
    token_weight = jnp.stack([chosen_weight, rejected_weight], axis=1)

    inputs = hidden_in[0].reshape(tokens, model_width)
    input_float = inputs.astype(jnp.float32)
    inverse_rms = lax.rsqrt(jnp.mean(input_float * input_float, axis=-1, keepdims=True) + EPSILON)
    normed = (input_float * inverse_rms * gain_vector).astype(jnp.bfloat16)
    values = jnp.dot(normed, value_matrix, preferred_element_type=jnp.float32).astype(jnp.bfloat16)
    values_heads = values.reshape(micro_count * 2, sequence_length, value_heads, HEAD_DIM)
    mixed = jnp.einsum(
        "ckgst,ctke->cskge", pattern, values_heads, preferred_element_type=jnp.float32
    )
    mixed = mixed.astype(jnp.bfloat16).reshape(tokens, mixed_columns)

    top = (token_weight[..., None] * full_head_grad.astype(jnp.float32)).astype(jnp.bfloat16)
    top = top.reshape(tokens, model_width)

    upstream = top
    for turn in range(section_count):
        if turn > 0:
            route = [(i + 1, i) for i in range(section_count - 1)]
            incoming = lax.ppermute(new_rows, "pipe", route)
            upstream = jnp.where(section_index == section_count - 1, top, incoming)
        mixed_grad = jnp.einsum(
            "sd,hd->sh", upstream, output_matrix, preferred_element_type=jnp.float32
        ).astype(jnp.bfloat16)
        mixed_heads = mixed_grad.reshape(
            micro_count * 2, sequence_length, value_heads, group_size, HEAD_DIM
        )
        values_grad = jnp.einsum(
            "ckgst,cskge->ctke", pattern, mixed_heads, preferred_element_type=jnp.float32
        )
        values_grad = values_grad.astype(jnp.bfloat16).reshape(tokens, value_columns)
        normed_grad = jnp.zeros((tokens, model_width), jnp.float32)
        for grad, matrix in zip([values_grad] + others(values_grad, "tensor"), value_matrices):
            term = jnp.einsum("sk,dk->sd", grad, matrix, preferred_element_type=jnp.float32)
            normed_grad = normed_grad + term.astype(jnp.bfloat16).astype(jnp.float32)
        scaled = normed_grad * gain_vector
        cubed = inverse_rms * inverse_rms * inverse_rms
        input_grad = inverse_rms * scaled - input_float * cubed * jnp.mean(
            input_float * scaled, axis=-1, keepdims=True
        )
        new_rows = (upstream.astype(jnp.float32) + input_grad).astype(jnp.bfloat16)

    gain_part = jnp.sum(normed_grad * input_float * inverse_rms, axis=0)
    value_part = jnp.einsum("sd,sk->dk", normed, values_grad, preferred_element_type=jnp.float32)
    rows = model_width // dp_count
    mixed_share, value_share, gain_rows = gradients(
        "dp",
        mixed,
        upstream.T.reshape(dp_count, rows, tokens),
        value_part.astype(jnp.bfloat16).reshape(dp_count, rows, value_columns),
        gain_part.reshape(dp_count, 1, rows),
    )
    own_output = lax.dynamic_slice_in_dim(
        new_rows.reshape(micro_count, 2, sequence_length, model_width),
        tensor_index * own_rows,
        own_rows,
        1,
    )
    return (own_output[None], value_share[None], mixed_share[None], gain_rows)


def solution(mesh):
    in_specs = (
        P("pipe", "dp", None, None, None),
        P("pipe", "dp", None, "tensor", None, None),
        P("pipe", None),
        P("pipe", None, "tensor"),
        P("pipe", "tensor", None),
        P("dp", "tensor", None, None),
        P("dp", None, None),
        P("dp", None),
        P("dp", None),
    )
    out_specs = (
        P("pipe", "dp", "tensor", None, None),
        P("pipe", "dp", "tensor"),
        P("pipe", "dp", "tensor"),
        P("pipe", "dp"),
    )
    return jax.shard_map(body, mesh=mesh, in_specs=in_specs, out_specs=out_specs, check_vma=False)
```

```python
import functools

import jax
import jax.numpy as jnp
from jax import lax
from jax.experimental import pallas as pl
from jax.experimental.pallas import tpu as pltpu
from jax.sharding import PartitionSpec as P

HEAD_DIM = 128
MESH = pl.DeviceIdType.MESH

EPSILON = 1e-06
DPO_BETA = 0.25
LIKELIHOOD_COEF = 0.2


def greet(peers):
    barrier = pltpu.get_barrier_semaphore()
    total = 0
    for axis, n in peers:
        me = lax.axis_index(axis)

        @pl.loop(1, n)
        def _(k):
            pl.semaphore_signal(
                barrier, inc=1, device_id={axis: lax.rem(me + k, n)}, device_id_type=MESH
            )

        total += n - 1
    pl.semaphore_wait(barrier, total)


def remote(src, dst, send_sem, recv_sem, **device):
    return pltpu.make_async_remote_copy(
        src_ref=src,
        dst_ref=dst,
        send_sem=send_sem,
        recv_sem=recv_sem,
        device_id=device,
        device_id_type=MESH,
    )


def layer_kernel(
    sizes,
    scale,
    mixed_ref,
    pattern_ref,
    hidden_ref,
    rms_ref,
    gain_ref,
    wv_ref,
    wo_hbm,
    head_ref,
    base_ref,
    mask_ref,
    count_ref,
    all_ref,
    dy_ref,
    rows_ref,
    grad_ref,
    gain_part_ref,
    wo_ref,
    wv_in,
    head_in,
    grad_in,
    count_in,
    wo_sem,
    z_send,
    z_recv,
    y_send,
    y_recv,
    c_send,
    c_recv,
    x_send,
    x_recv,
    p_send,
    p_recv,
):
    n, nt, np_ = sizes
    me, ti, pi = lax.axis_index("dp"), lax.axis_index("tensor"), lax.axis_index("pipe")
    fast = 2 if n % 2 == 0 else 1
    slow = n // fast
    partner = me + 1 - 2 * lax.rem(me, 2)
    last = pi == np_ - 1
    wo_copy = pltpu.make_async_copy(wo_hbm, wo_ref, wo_sem)
    wo_copy.start()
    greet((("dp", n), ("tensor", nt), ("pipe", np_)))

    def head_copy(k):
        peer = lax.rem(ti + k, nt)
        return remote(head_ref, head_in.at[k], x_send.at[0, k], x_recv.at[0, k], tensor=peer)

    def wv_copy(k):
        peer = lax.rem(ti + k, nt)
        return remote(wv_ref, wv_in.at[k], x_send.at[1, k], x_recv.at[1, k], tensor=peer)

    def grad_copy(k):
        peer = lax.rem(ti + k, nt)
        return remote(grad_ref, grad_in.at[k], x_send.at[2, k], x_recv.at[2, k], tensor=peer)

    def count_copy(k):
        return remote(
            count_ref, count_in.at[k], c_send.at[k], c_recv.at[k], dp=lax.rem(me + k, n)
        )

    def z_copy(k):
        return remote(
            mixed_ref, all_ref.at[me], z_send.at[k], z_recv.at[k], dp=lax.rem(me + fast * k, n)
        )

    def y_copy(k):
        src = lax.rem(me - fast * k + n, n)
        block = mixed_ref if isinstance(k, int) and k == 0 else all_ref.at[src]
        return remote(block, all_ref.at[src], y_send.at[k], y_recv.at[k], dp=partner)

    def forward(low, high):
        @pl.loop(low, high)
        def _(k):
            z_copy(k).wait_recv()
            if fast > 1:
                y_copy(k).start()

    for k in range(1, n):
        count_copy(k).start()

    @pl.when(last)
    def _():
        for k in range(1, nt):
            head_copy(k).start()

    for k in range(1, nt):
        wv_copy(k).start()
    if fast > 1:
        y_copy(0).start()

    @pl.loop(1, slow)
    def _(k):
        z_copy(k).start()

    all_ref[me] = mixed_ref[...]
    total = count_ref[0:1, 0:1]
    for k in range(1, n):
        count_copy(k).wait_recv()
        total = total + count_in[k, 0:1, 0:1]
    likelihood = scale / total.astype(jnp.float32)
    wo_copy.wait()

    micro, own, length = head_ref.shape[:3]
    tokens = dy_ref.shape[0]
    sequences = tokens // length
    heads = pattern_ref.shape[1] // length

    @pl.when(last)
    def _():
        for k in range(nt):
            if k > 0:
                head_copy(k).wait_recv()
            origin = lax.rem(ti - k + nt, nt)
            for p in range(micro):
                for r in range(own):
                    start = pl.multiple_of((p * nt * own + origin * own + r) * length, length)
                    at = pl.ds(start, length)
                    weight = base_ref[at, :] - likelihood * mask_ref[at, :]
                    block = (head_ref if k == 0 else head_in.at[k])[p, r]
                    dy_ref[at, :] = (weight * block.astype(jnp.float32)).astype(jnp.bfloat16)

    def down_copy():
        return remote(rows_ref, dy_ref, p_send.at[0], p_recv.at[0], pipe=lax.rem(pi - 1 + np_, np_))

    if np_ > 1:

        @pl.when(jnp.logical_not(last))
        def _():
            forward(1, slow - 1)
            down_copy().wait_recv()

    mixed_grad = lax.dot_general(
        dy_ref[...],
        wo_ref[...],
        (((1,), (1,)), ((), ())),
        preferred_element_type=jnp.float32,
    ).astype(jnp.bfloat16)
    per_value = heads // (grad_ref.shape[1] // HEAD_DIM)
    for c in range(sequences):
        at = slice(c * length, (c + 1) * length)
        for v in range(grad_ref.shape[1] // HEAD_DIM):
            stacked = jnp.concatenate(
                [
                    mixed_grad[at, h * HEAD_DIM : (h + 1) * HEAD_DIM]
                    for h in range(v * per_value, (v + 1) * per_value)
                ],
                axis=0,
            )
            pattern = pattern_ref[c, v * per_value * length : (v + 1) * per_value * length, :]
            grad_ref[at, v * HEAD_DIM : (v + 1) * HEAD_DIM] = lax.dot_general(
                pattern, stacked, (((0,), (0,)), ((), ())), preferred_element_type=jnp.float32
            ).astype(jnp.bfloat16)
    for k in range(1, nt):
        grad_copy(k).start()

    @pl.when(last)
    def _():
        forward(1, min(2, slow))

    if np_ > 1:

        @pl.when(jnp.logical_not(last))
        def _():
            forward(max(1, slow - 1), slow)

    for k in range(1, nt):
        wv_copy(k).wait_recv()
        grad_copy(k).wait_recv()
    gain_part_ref[...] = jnp.zeros_like(gain_part_ref)

    @pl.loop(0, sequences)
    def _(c):
        at = pl.ds(pl.multiple_of(c * length, length), length)
        normed_grad = jnp.zeros((length, dy_ref.shape[1]), jnp.float32)
        for k in range(nt):
            grad = grad_ref[at, :] if k == 0 else grad_in[k, at, :]
            matrix = wv_ref[...] if k == 0 else wv_in[k]
            term = lax.dot_general(
                grad, matrix, (((1,), (1,)), ((), ())), preferred_element_type=jnp.float32
            )
            normed_grad = normed_grad + term.astype(jnp.bfloat16).astype(jnp.float32)
        x = hidden_ref[at, :].astype(jnp.float32)
        rms = rms_ref[at, :]
        scaled = normed_grad * gain_ref[...]
        gain_part_ref[...] += jnp.sum(normed_grad * x * rms, axis=0, keepdims=True)
        mean = jnp.mean(x * scaled, axis=-1, keepdims=True)
        input_grad = rms * scaled - x * (rms * rms * rms * mean)
        rows_ref[at, :] = (dy_ref[at, :].astype(jnp.float32) + input_grad).astype(jnp.bfloat16)

    if np_ > 1:

        @pl.when(pi > 0)
        def _():
            down_copy().start()

    @pl.when(last)
    def _():
        forward(min(2, slow), slow)

    if fast > 1:
        y_copy(0).wait()

        @pl.loop(1, slow)
        def _(k):
            y_copy(k).wait()

    @pl.loop(1, slow)
    def _(k):
        z_copy(k).wait_send()

    for k in range(1, n):
        count_copy(k).wait_send()
    for k in range(1, nt):
        wv_copy(k).wait_send()
        grad_copy(k).wait_send()

    @pl.when(last)
    def _():
        for k in range(1, nt):
            head_copy(k).wait_send()

    if np_ > 1:

        @pl.when(pi > 0)
        def _():
            down_copy().wait_send()


def layer(sizes, scale, mixed, pattern, hidden, rms, gain, wv, wo, head, base, mask, count):
    n, nt, _ = sizes
    tokens, width = hidden.shape
    vmem = pl.BlockSpec(memory_space=pltpu.VMEM)
    dma = pltpu.SemaphoreType.DMA
    return pl.pallas_call(
        functools.partial(layer_kernel, sizes, scale),
        out_shape=(
            jax.ShapeDtypeStruct((n,) + mixed.shape, jnp.bfloat16),
            jax.ShapeDtypeStruct((tokens, width), jnp.bfloat16),
            jax.ShapeDtypeStruct((tokens, width), jnp.bfloat16),
            jax.ShapeDtypeStruct((tokens, wv.shape[1]), jnp.bfloat16),
            jax.ShapeDtypeStruct((1, width), jnp.float32),
        ),
        in_specs=[vmem] * 6 + [pl.BlockSpec(memory_space=pl.ANY)] + [vmem] * 4,
        out_specs=(vmem,) * 5,
        scratch_shapes=[
            pltpu.VMEM(wo.shape, jnp.bfloat16),
            pltpu.VMEM((nt,) + wv.shape, jnp.bfloat16),
            pltpu.VMEM((nt,) + head.shape, jnp.bfloat16),
            pltpu.VMEM((nt, tokens, wv.shape[1]), jnp.bfloat16),
            pltpu.VMEM((n,) + count.shape, jnp.int32),
            dma,
            dma((n,)),
            dma((n,)),
            dma((n,)),
            dma((n,)),
            dma((n,)),
            dma((n,)),
            dma((3, nt)),
            dma((3, nt)),
            dma((1,)),
            dma((1,)),
        ],
        compiler_params=pltpu.CompilerParams(
            collective_id=0, has_side_effects=True, vmem_limit_bytes=63 * 2**20
        ),
        name="layer",
    )(mixed, pattern, hidden, rms, gain, wv, wo, head, base, mask, count)


def gradient_kernel(
    sizes,
    mixed_ref,
    dy_ref,
    value_ref,
    gain_ref,
    out_ref,
    value_out_ref,
    gain_out_ref,
    dy_in,
    value_in,
    gain_in,
    send_sem,
    recv_sem,
    x_send,
    x_recv,
):
    n, nt = sizes
    me, ti = lax.axis_index("dp"), lax.axis_index("tensor")
    part = dy_ref.shape[3]
    greet((("dp", n), ("tensor", nt)))

    def copies(k):
        peer = lax.rem(me + k, n)
        pairs = (
            (dy_ref.at[ti, peer], dy_in.at[ti, k]),
            (value_ref.at[peer], value_in.at[k]),
            (gain_ref.at[peer], gain_in.at[k]),
        )
        return [
            remote(src, dst, send_sem.at[i, k], recv_sem.at[i, k], dp=peer)
            for i, (src, dst) in enumerate(pairs)
        ]

    def onward(j, k):
        block = dy_in.at[ti, k]
        return remote(block, block, x_send.at[j, k], x_recv.at[j, k], tensor=lax.rem(ti + j, nt))

    def product(dy, owner, half):
        at = pl.ds(pl.multiple_of(half * part, part), part)
        return jnp.dot(dy, mixed_ref[owner, at, :], preferred_element_type=jnp.float32)

    @pl.loop(1, n)
    def _(k):
        copies(k)[0].start()

    @pl.loop(1, n)
    def _(k):
        for c in copies(k)[1:]:
            c.start()

    out_ref[...] = product(dy_ref[0, me], me, 0)
    for half in range(1, nt):
        out_ref[...] += product(dy_ref[half, me], me, half)
    value_out_ref[...] = value_ref[me].astype(jnp.float32)
    gain_out_ref[...] = gain_ref[me]

    @pl.loop(1, n)
    def _(k):
        copies(k)[0].wait_recv()
        for j in range(1, nt):
            onward(j, k).start()
        out_ref[...] += product(dy_in[ti, k], lax.rem(me - k + n, n), ti)

    @pl.loop(1, n)
    def _(k):
        for j in range(1, nt):
            half = lax.rem(ti - j + nt, nt)
            remote(
                dy_in.at[half, k], dy_in.at[half, k], x_send.at[j, k], x_recv.at[j, k],
                tensor=lax.rem(ti + j, nt),
            ).wait_recv()
            out_ref[...] += product(dy_in[half, k], lax.rem(me - k + n, n), half)

    @pl.loop(1, n)
    def _(k):
        for c in copies(k)[1:]:
            c.wait_recv()
        value_out_ref[...] += value_in[k].astype(jnp.float32)
        gain_out_ref[...] += gain_in[k]

    @pl.loop(1, n)
    def _(k):
        for c in copies(k):
            c.wait_send()
        for j in range(1, nt):
            onward(j, k).wait_send()


def gradients(mixed_all, dy, value_part, gain_part):
    nt, n, rows, part = dy.shape
    columns, value_columns = mixed_all.shape[2], value_part.shape[2]
    vmem = pl.BlockSpec(memory_space=pltpu.VMEM)
    return pl.pallas_call(
        functools.partial(gradient_kernel, (n, nt)),
        out_shape=(
            jax.ShapeDtypeStruct((rows, columns), jnp.float32),
            jax.ShapeDtypeStruct((rows, value_columns), jnp.float32),
            jax.ShapeDtypeStruct((1, rows), jnp.float32),
        ),
        in_specs=[vmem] * 4,
        out_specs=(vmem,) * 3,
        scratch_shapes=[
            pltpu.VMEM((nt, n, rows, part), jnp.bfloat16),
            pltpu.VMEM((n, rows, value_columns), jnp.bfloat16),
            pltpu.VMEM((n, 1, rows), jnp.float32),
            pltpu.SemaphoreType.DMA((3, n)),
            pltpu.SemaphoreType.DMA((3, n)),
            pltpu.SemaphoreType.DMA((nt, n)),
            pltpu.SemaphoreType.DMA((nt, n)),
        ],
        compiler_params=pltpu.CompilerParams(
            collective_id=1, has_side_effects=True, vmem_limit_bytes=56 * 2**20
        ),
        name="gradients",
    )(mixed_all, dy, value_part, gain_part)


def body(
    hidden_in,
    attention_probs,
    norm_gain,
    value_weight,
    output_weight,
    head_grad,
    policy_logprob,
    reference_logprob,
    sequence_bounds,
):
    tensor_index = lax.axis_index("tensor")
    tensor_count = lax.axis_size("tensor")
    dp_count = lax.axis_size("dp")
    micro_count, _, sequence_length, model_width = hidden_in.shape[1:]
    tokens = micro_count * 2 * sequence_length
    value_columns = value_weight.shape[2]
    value_heads = value_columns // HEAD_DIM
    local_heads = attention_probs.shape[3]
    group_size = local_heads // value_heads
    mixed_columns = output_weight.shape[1]
    own_rows = 2 // tensor_count
    value_matrix = value_weight[0]
    pattern = attention_probs[0].reshape(
        micro_count * 2, value_heads, group_size, sequence_length, sequence_length
    )
    positions = jnp.arange(sequence_length, dtype=jnp.int32)
    response_bool = (positions[None, None, :] >= sequence_bounds[:, 0:1, None]) & (
        positions[None, None, :] < sequence_bounds[:, 1:3, None]
    )
    local_count = jnp.sum(response_bool[:, 0, :].astype(jnp.int32))
    response_mask = response_bool.astype(jnp.float32)
    sequence_logprob = jnp.sum(response_mask * policy_logprob, axis=-1)
    margin = DPO_BETA * (
        sequence_logprob[:, 0]
        - reference_logprob[:, 0]
        - (sequence_logprob[:, 1] - reference_logprob[:, 1])
    )
    weight_pair = jax.nn.sigmoid(-margin)
    sign = jnp.array([-DPO_BETA, DPO_BETA], jnp.float32)
    base_weight = sign[None, :, None] * weight_pair[:, None, None] * response_mask
    chosen_mask = response_mask * jnp.array([1.0, 0.0], jnp.float32)[None, :, None]

    inputs = hidden_in[0].reshape(tokens, model_width)
    input_float = inputs.astype(jnp.float32)
    inverse_rms = lax.rsqrt(jnp.mean(input_float * input_float, axis=-1, keepdims=True) + EPSILON)
    normed = (input_float * inverse_rms * norm_gain).astype(jnp.bfloat16)
    values = jnp.dot(normed, value_matrix, preferred_element_type=jnp.float32).astype(jnp.bfloat16)
    values_heads = values.reshape(micro_count * 2, sequence_length, value_heads, HEAD_DIM)
    mixed = jnp.einsum(
        "ckgst,ctke->cskge", pattern, values_heads, preferred_element_type=jnp.float32
    )
    mixed = mixed.astype(jnp.bfloat16).reshape(tokens, mixed_columns)

    mixed_all, upstream, new_rows, values_grad, gain_part = layer(
        (dp_count, tensor_count, lax.axis_size("pipe")),
        LIKELIHOOD_COEF * micro_count * dp_count,
        mixed,
        pattern.reshape(micro_count * 2, local_heads * sequence_length, sequence_length),
        inputs,
        inverse_rms,
        norm_gain,
        value_matrix,
        output_weight[0],
        head_grad,
        base_weight.reshape(tokens, 1),
        chosen_mask.reshape(tokens, 1),
        jnp.broadcast_to(local_count, (8, 128)),
    )
    value_part = jnp.einsum("sd,sk->dk", normed, values_grad, preferred_element_type=jnp.float32)
    rows = model_width // dp_count
    halves = upstream.reshape(tensor_count, tokens // tensor_count, dp_count, rows)
    mixed_share, value_share, gain_rows = gradients(
        mixed_all,
        halves.transpose(0, 2, 3, 1),
        value_part.astype(jnp.bfloat16).reshape(dp_count, rows, value_columns),
        gain_part.reshape(dp_count, 1, rows),
    )
    own_output = lax.dynamic_slice_in_dim(
        new_rows.reshape(micro_count, 2, sequence_length, model_width),
        tensor_index * own_rows,
        own_rows,
        1,
    )
    return (own_output[None], value_share[None], mixed_share[None], gain_rows)


def solution(mesh):
    in_specs = (
        P("pipe", "dp", None, None, None),
        P("pipe", "dp", None, "tensor", None, None),
        P("pipe", None),
        P("pipe", None, "tensor"),
        P("pipe", "tensor", None),
        P("dp", "tensor", None, None),
        P("dp", None, None),
        P("dp", None),
        P("dp", None),
    )
    out_specs = (
        P("pipe", "dp", "tensor", None, None),
        P("pipe", "dp", "tensor"),
        P("pipe", "dp", "tensor"),
        P("pipe", "dp"),
    )
    return jax.shard_map(body, mesh=mesh, in_specs=in_specs, out_specs=out_specs, check_vma=False)
```

```python
import functools

import jax
import jax.numpy as jnp
from jax import lax
from jax.experimental import pallas as pl
from jax.experimental.pallas import tpu as pltpu
from jax.sharding import PartitionSpec as P

HEAD_DIM = 128
MESH = pl.DeviceIdType.MESH

EPSILON = 1e-06
DPO_BETA = 0.25
LIKELIHOOD_COEF = 0.2


def greet(peers):
    barrier = pltpu.get_barrier_semaphore()
    total = 0
    for axis, n in peers:
        me = lax.axis_index(axis)

        @pl.loop(1, n)
        def _(k):
            pl.semaphore_signal(
                barrier, inc=1, device_id={axis: lax.rem(me + k, n)}, device_id_type=MESH
            )

        total += n - 1
    pl.semaphore_wait(barrier, total)


def remote(src, dst, send_sem, recv_sem, **device):
    return pltpu.make_async_remote_copy(
        src_ref=src,
        dst_ref=dst,
        send_sem=send_sem,
        recv_sem=recv_sem,
        device_id=device,
        device_id_type=MESH,
    )


def layer_kernel(
    sizes,
    scale,
    pack_ref,
    pattern_ref,
    hidden_ref,
    rms_ref,
    gain_ref,
    wv_ref,
    wo_hbm,
    head_ref,
    base_ref,
    mask_ref,
    count_ref,
    all_ref,
    turned_ref,
    rows_ref,
    grad_ref,
    gain_part_ref,
    dy_ref,
    wo_ref,
    wv_in,
    head_in,
    grad_in,
    count_in,
    wo_sem,
    z_send,
    z_recv,
    y_send,
    y_recv,
    c_send,
    c_recv,
    x_send,
    x_recv,
    p_send,
    p_recv,
):
    n, nt, np_ = sizes
    me, ti, pi = lax.axis_index("dp"), lax.axis_index("tensor"), lax.axis_index("pipe")
    fast = 2 if n % 2 == 0 else 1
    slow = n // fast
    partner = me + 1 - 2 * lax.rem(me, 2)
    last = pi == np_ - 1
    wo_copy = pltpu.make_async_copy(wo_hbm, wo_ref, wo_sem)
    wo_copy.start()
    greet((("dp", n), ("tensor", nt), ("pipe", np_)))

    def head_copy(k):
        peer = lax.rem(ti + k, nt)
        return remote(head_ref, head_in.at[k], x_send.at[0, k], x_recv.at[0, k], tensor=peer)

    def wv_copy(k):
        peer = lax.rem(ti + k, nt)
        return remote(wv_ref, wv_in.at[k], x_send.at[1, k], x_recv.at[1, k], tensor=peer)

    def grad_copy(k):
        peer = lax.rem(ti + k, nt)
        return remote(grad_ref, grad_in.at[k], x_send.at[2, k], x_recv.at[2, k], tensor=peer)

    def count_copy(k):
        return remote(
            count_ref, count_in.at[k], c_send.at[k], c_recv.at[k], dp=lax.rem(me + k, n)
        )

    def z_copy(k):
        return remote(
            pack_ref, all_ref.at[me], z_send.at[k], z_recv.at[k], dp=lax.rem(me + fast * k, n)
        )

    def y_copy(k):
        src = lax.rem(me - fast * k + n, n)
        block = pack_ref if isinstance(k, int) and k == 0 else all_ref.at[src]
        return remote(block, all_ref.at[src], y_send.at[k], y_recv.at[k], dp=partner)

    def forward(low, high):
        @pl.loop(low, high)
        def _(k):
            z_copy(k).wait_recv()
            if fast > 1:
                y_copy(k).start()

    for k in range(1, n):
        count_copy(k).start()

    @pl.when(last)
    def _():
        for k in range(1, nt):
            head_copy(k).start()

    for k in range(1, nt):
        wv_copy(k).start()
    if fast > 1:
        y_copy(0).start()

    @pl.loop(1, slow)
    def _(k):
        z_copy(k).start()

    all_ref[me] = pack_ref[...]
    total = count_ref[0:1, 0:1]
    for k in range(1, n):
        count_copy(k).wait_recv()
        total = total + count_in[k, 0:1, 0:1]
    likelihood = scale / total.astype(jnp.float32)
    wo_copy.wait()

    micro, own, length = head_ref.shape[:3]
    tokens = dy_ref.shape[0]
    sequences = tokens // length
    heads = pattern_ref.shape[1] // length

    @pl.when(last)
    def _():
        for k in range(nt):
            if k > 0:
                head_copy(k).wait_recv()
            origin = lax.rem(ti - k + nt, nt)
            for p in range(micro):
                for r in range(own):
                    start = pl.multiple_of((p * nt * own + origin * own + r) * length, length)
                    at = pl.ds(start, length)
                    weight = base_ref[at, :] - likelihood * mask_ref[at, :]
                    block = (head_ref if k == 0 else head_in.at[k])[p, r]
                    dy_ref[at, :] = (weight * block.astype(jnp.float32)).astype(jnp.bfloat16)

    def down_copy():
        return remote(rows_ref, dy_ref, p_send.at[0], p_recv.at[0], pipe=lax.rem(pi - 1 + np_, np_))

    if np_ > 1:

        @pl.when(jnp.logical_not(last))
        def _():
            forward(1, slow - 1)
            down_copy().wait_recv()

    mixed_grad = lax.dot_general(
        dy_ref[...],
        wo_ref[...],
        (((1,), (1,)), ((), ())),
        preferred_element_type=jnp.float32,
    ).astype(jnp.bfloat16)
    per_value = heads // (grad_ref.shape[1] // HEAD_DIM)
    for c in range(sequences):
        at = slice(c * length, (c + 1) * length)
        for v in range(grad_ref.shape[1] // HEAD_DIM):
            stacked = jnp.concatenate(
                [
                    mixed_grad[at, h * HEAD_DIM : (h + 1) * HEAD_DIM]
                    for h in range(v * per_value, (v + 1) * per_value)
                ],
                axis=0,
            )
            pattern = pattern_ref[c, v * per_value * length : (v + 1) * per_value * length, :]
            grad_ref[at, v * HEAD_DIM : (v + 1) * HEAD_DIM] = lax.dot_general(
                pattern, stacked, (((0,), (0,)), ((), ())), preferred_element_type=jnp.float32
            ).astype(jnp.bfloat16)
    for k in range(1, nt):
        grad_copy(k).start()

    @pl.when(last)
    def _():
        forward(1, min(2, slow))

    if np_ > 1:

        @pl.when(jnp.logical_not(last))
        def _():
            forward(max(1, slow - 1), slow)

    for k in range(1, nt):
        wv_copy(k).wait_recv()
        grad_copy(k).wait_recv()
    gain_part_ref[...] = jnp.zeros_like(gain_part_ref)

    @pl.loop(0, sequences)
    def _(c):
        at = pl.ds(pl.multiple_of(c * length, length), length)
        normed_grad = jnp.zeros((length, dy_ref.shape[1]), jnp.float32)
        for k in range(nt):
            grad = grad_ref[at, :] if k == 0 else grad_in[k, at, :]
            matrix = wv_ref[...] if k == 0 else wv_in[k]
            term = lax.dot_general(
                grad, matrix, (((1,), (1,)), ((), ())), preferred_element_type=jnp.float32
            )
            normed_grad = normed_grad + term.astype(jnp.bfloat16).astype(jnp.float32)
        x = hidden_ref[at, :].astype(jnp.float32)
        rms = rms_ref[at, :]
        scaled = normed_grad * gain_ref[...]
        gain_part_ref[...] += jnp.sum(normed_grad * x * rms, axis=0, keepdims=True)
        mean = jnp.mean(x * scaled, axis=-1, keepdims=True)
        input_grad = rms * scaled - x * (rms * rms * rms * mean)
        rows_ref[at, :] = (dy_ref[at, :].astype(jnp.float32) + input_grad).astype(jnp.bfloat16)

    if np_ > 1:

        @pl.when(pi > 0)
        def _():
            down_copy().start()

    @pl.loop(0, dy_ref.shape[1] // 128)
    def _(j):
        at = pl.ds(pl.multiple_of(j * 128, 128), 128)
        turned_ref[at, :] = dy_ref[:, at].T

    @pl.when(last)
    def _():
        forward(min(2, slow), slow)

    if fast > 1:
        y_copy(0).wait()

        @pl.loop(1, slow)
        def _(k):
            y_copy(k).wait()

    @pl.loop(1, slow)
    def _(k):
        z_copy(k).wait_send()

    for k in range(1, n):
        count_copy(k).wait_send()
    for k in range(1, nt):
        wv_copy(k).wait_send()
        grad_copy(k).wait_send()

    @pl.when(last)
    def _():
        for k in range(1, nt):
            head_copy(k).wait_send()

    if np_ > 1:

        @pl.when(pi > 0)
        def _():
            down_copy().wait_send()


def layer(sizes, scale, mixed, pattern, hidden, rms, gain, wv, wo, head, base, mask, count):
    n, nt, _ = sizes
    tokens, width = hidden.shape
    vmem = pl.BlockSpec(memory_space=pltpu.VMEM)
    dma = pltpu.SemaphoreType.DMA
    return pl.pallas_call(
        functools.partial(layer_kernel, sizes, scale),
        out_shape=(
            jax.ShapeDtypeStruct((n,) + mixed.shape, jnp.bfloat16),
            jax.ShapeDtypeStruct((width, tokens), jnp.bfloat16),
            jax.ShapeDtypeStruct((tokens, width), jnp.bfloat16),
            jax.ShapeDtypeStruct((tokens, wv.shape[1]), jnp.bfloat16),
            jax.ShapeDtypeStruct((1, width), jnp.float32),
        ),
        in_specs=[vmem] * 6 + [pl.BlockSpec(memory_space=pl.ANY)] + [vmem] * 4,
        out_specs=(vmem,) * 5,
        scratch_shapes=[
            pltpu.VMEM((tokens, width), jnp.bfloat16),
            pltpu.VMEM(wo.shape, jnp.bfloat16),
            pltpu.VMEM((nt,) + wv.shape, jnp.bfloat16),
            pltpu.VMEM((nt,) + head.shape, jnp.bfloat16),
            pltpu.VMEM((nt, tokens, wv.shape[1]), jnp.bfloat16),
            pltpu.VMEM((n,) + count.shape, jnp.int32),
            dma,
            dma((n,)),
            dma((n,)),
            dma((n,)),
            dma((n,)),
            dma((n,)),
            dma((n,)),
            dma((3, nt)),
            dma((3, nt)),
            dma((1,)),
            dma((1,)),
        ],
        compiler_params=pltpu.CompilerParams(
            collective_id=0, has_side_effects=True, vmem_limit_bytes=63 * 2**20
        ),
        name="layer",
    )(mixed, pattern, hidden, rms, gain, wv, wo, head, base, mask, count)


def gradient_kernel(
    sizes,
    length,
    pack_ref,
    dy_ref,
    value_ref,
    gain_ref,
    out_ref,
    value_out_ref,
    gain_out_ref,
    mixed_ref,
    dy_in,
    near_in,
    near_sum,
    value_in,
    gain_in,
    send_sem,
    recv_sem,
    x_send,
    x_recv,
    near_sem,
):
    n, nt = sizes
    me, ti = lax.axis_index("dp"), lax.axis_index("tensor")
    part = dy_in.shape[3]
    slow, fast = value_ref.shape[:2]
    line, side = lax.div(me, fast), lax.rem(me, fast)
    partner = me + 1 - 2 * side
    greet((("dp", n), ("tensor", nt)))

    def half_of(half):
        return pl.ds(pl.multiple_of(half * part, part), part)

    def near_copy():
        return remote(
            value_ref.at[:, fast - 1 - side], near_in, near_sem.at[0], near_sem.at[1], dp=partner
        )

    def value_copy(k):
        return remote(
            near_sum.at[lax.rem(line + k, slow)],
            value_in.at[k],
            send_sem.at[2, k],
            recv_sem.at[2, k],
            dp=lax.rem(me + fast * k, n),
        )

    def copies(k):
        peer = lax.rem(me + k, n)
        pairs = (
            (dy_ref.at[peer, :, half_of(ti)], dy_in.at[ti, k]),
            (gain_ref.at[peer], gain_in.at[k]),
        )
        return [
            remote(src, dst, send_sem.at[i, k], recv_sem.at[i, k], dp=peer)
            for i, (src, dst) in enumerate(pairs)
        ]

    def onward(j, k):
        block = dy_in.at[ti, k]
        return remote(block, block, x_send.at[j, k], x_recv.at[j, k], tensor=lax.rem(ti + j, nt))

    def product(dy, owner, half):
        return jnp.dot(dy, mixed_ref[owner, half_of(half), :], preferred_element_type=jnp.float32)

    if fast > 1:
        near_copy().start()

    @pl.loop(1, n)
    def _(k):
        for c in copies(k):
            c.start()

    if fast > 1:
        near_copy().wait_recv()

    @pl.loop(0, slow)
    def _(j):
        near = value_ref[j, side].astype(jnp.float32)
        if fast > 1:
            near = near + near_in[j].astype(jnp.float32)
        near_sum[j] = near.astype(jnp.bfloat16)

    @pl.loop(1, slow)
    def _(k):
        value_copy(k).start()

    heads, tokens = mixed_ref.shape[2] // HEAD_DIM, mixed_ref.shape[1]
    per_value = heads // (value_ref.shape[3] // HEAD_DIM)
    both = 2 * length
    owner_of = lax.broadcasted_iota(jnp.int32, (both, HEAD_DIM), 0) // length

    @pl.loop(0, n)
    def _(src):
        for p in range(tokens // both):
            for v in range(heads // per_value):
                first = (p * heads + v * per_value) * length
                pattern = pack_ref[src, first : first + per_value * length, :]
                first = tokens // 2 * heads + v * tokens + p * both
                values = pack_ref[src, first : first + both, :]
                for c in range(2):
                    mixed = jnp.dot(
                        pattern,
                        jnp.where(owner_of == c, values, jnp.zeros_like(values)),
                        preferred_element_type=jnp.float32,
                    ).astype(jnp.bfloat16)
                    row = (p * 2 + c) * length
                    for h in range(per_value):
                        column = (v * per_value + h) * HEAD_DIM
                        mixed_ref[src, row : row + length, column : column + HEAD_DIM] = mixed[
                            h * length : (h + 1) * length
                        ]

    out_ref[...] = jnp.dot(dy_ref[me], mixed_ref[me], preferred_element_type=jnp.float32)
    value_out_ref[...] = near_sum[line].astype(jnp.float32)
    gain_out_ref[...] = gain_ref[me]

    @pl.loop(1, n)
    def _(k):
        copies(k)[0].wait_recv()
        for j in range(1, nt):
            onward(j, k).start()
        out_ref[...] += product(dy_in[ti, k], lax.rem(me - k + n, n), ti)

    @pl.loop(1, n)
    def _(k):
        for j in range(1, nt):
            half = lax.rem(ti - j + nt, nt)
            remote(
                dy_in.at[half, k], dy_in.at[half, k], x_send.at[j, k], x_recv.at[j, k],
                tensor=lax.rem(ti + j, nt),
            ).wait_recv()
            out_ref[...] += product(dy_in[half, k], lax.rem(me - k + n, n), half)

    @pl.loop(1, n)
    def _(k):
        copies(k)[1].wait_recv()
        gain_out_ref[...] += gain_in[k]

    @pl.loop(1, slow)
    def _(k):
        value_copy(k).wait_recv()
        value_out_ref[...] += value_in[k].astype(jnp.float32)

    @pl.loop(1, n)
    def _(k):
        for c in copies(k):
            c.wait_send()
        for j in range(1, nt):
            onward(j, k).wait_send()

    @pl.loop(1, slow)
    def _(k):
        value_copy(k).wait_send()

    if fast > 1:
        near_copy().wait_send()


def gradients(nt, length, columns, pack_all, dy, value_part, gain_part):
    n, rows, tokens = dy.shape
    part = tokens // nt
    slow, _, _, value_columns = value_part.shape
    vmem = pl.BlockSpec(memory_space=pltpu.VMEM)
    return pl.pallas_call(
        functools.partial(gradient_kernel, (n, nt), length),
        out_shape=(
            jax.ShapeDtypeStruct((rows, columns), jnp.float32),
            jax.ShapeDtypeStruct((rows, value_columns), jnp.float32),
            jax.ShapeDtypeStruct((1, rows), jnp.float32),
        ),
        in_specs=[vmem] * 4,
        out_specs=(vmem,) * 3,
        scratch_shapes=[
            pltpu.VMEM((n, tokens, columns), jnp.bfloat16),
            pltpu.VMEM((nt, n, rows, part), jnp.bfloat16),
            pltpu.VMEM((slow, rows, value_columns), jnp.bfloat16),
            pltpu.VMEM((slow, rows, value_columns), jnp.bfloat16),
            pltpu.VMEM((slow, rows, value_columns), jnp.bfloat16),
            pltpu.VMEM((n, 1, rows), jnp.float32),
            pltpu.SemaphoreType.DMA((3, n)),
            pltpu.SemaphoreType.DMA((3, n)),
            pltpu.SemaphoreType.DMA((nt, n)),
            pltpu.SemaphoreType.DMA((nt, n)),
            pltpu.SemaphoreType.DMA((2,)),
        ],
        compiler_params=pltpu.CompilerParams(
            collective_id=1, has_side_effects=True, vmem_limit_bytes=63 * 2**20
        ),
        name="gradients",
    )(pack_all, dy, value_part, gain_part)


def body(
    hidden_in,
    attention_probs,
    norm_gain,
    value_weight,
    output_weight,
    head_grad,
    policy_logprob,
    reference_logprob,
    sequence_bounds,
):
    tensor_index = lax.axis_index("tensor")
    tensor_count = lax.axis_size("tensor")
    dp_count = lax.axis_size("dp")
    micro_count, _, sequence_length, model_width = hidden_in.shape[1:]
    tokens = micro_count * 2 * sequence_length
    value_columns = value_weight.shape[2]
    value_heads = value_columns // HEAD_DIM
    local_heads = attention_probs.shape[3]
    own_rows = 2 // tensor_count
    value_matrix = value_weight[0]
    positions = jnp.arange(sequence_length, dtype=jnp.int32)
    response_bool = (positions[None, None, :] >= sequence_bounds[:, 0:1, None]) & (
        positions[None, None, :] < sequence_bounds[:, 1:3, None]
    )
    local_count = jnp.sum(response_bool[:, 0, :].astype(jnp.int32))
    response_mask = response_bool.astype(jnp.float32)
    sequence_logprob = jnp.sum(response_mask * policy_logprob, axis=-1)
    margin = DPO_BETA * (
        sequence_logprob[:, 0]
        - reference_logprob[:, 0]
        - (sequence_logprob[:, 1] - reference_logprob[:, 1])
    )
    weight_pair = jax.nn.sigmoid(-margin)
    sign = jnp.array([-DPO_BETA, DPO_BETA], jnp.float32)
    base_weight = sign[None, :, None] * weight_pair[:, None, None] * response_mask
    chosen_mask = response_mask * jnp.array([1.0, 0.0], jnp.float32)[None, :, None]

    inputs = hidden_in[0].reshape(tokens, model_width)
    input_float = inputs.astype(jnp.float32)
    inverse_rms = lax.rsqrt(jnp.mean(input_float * input_float, axis=-1, keepdims=True) + EPSILON)
    normed = (input_float * inverse_rms * norm_gain).astype(jnp.bfloat16)
    values = jnp.dot(normed, value_matrix, preferred_element_type=jnp.float32).astype(jnp.bfloat16)
    pairs = attention_probs[0].transpose(0, 2, 3, 1, 4).reshape(-1, 2 * sequence_length)
    heads = values.reshape(tokens, value_heads, HEAD_DIM).transpose(1, 0, 2).reshape(-1, HEAD_DIM)
    pack = jnp.concatenate([pairs, heads], axis=0)

    pack_all, turned, new_rows, values_grad, gain_part = layer(
        (dp_count, tensor_count, lax.axis_size("pipe")),
        LIKELIHOOD_COEF * micro_count * dp_count,
        pack,
        attention_probs[0].reshape(
            micro_count * 2, local_heads * sequence_length, sequence_length
        ),
        inputs,
        inverse_rms,
        norm_gain,
        value_matrix,
        output_weight[0],
        head_grad,
        base_weight.reshape(tokens, 1),
        chosen_mask.reshape(tokens, 1),
        jnp.broadcast_to(local_count, (8, 128)),
    )
    value_part = jnp.einsum("sd,sk->dk", normed, values_grad, preferred_element_type=jnp.float32)
    rows = model_width // dp_count
    fast = 2 if dp_count % 2 == 0 else 1
    mixed_share, value_share, gain_rows = gradients(
        tensor_count,
        sequence_length,
        output_weight.shape[1],
        pack_all,
        turned.reshape(dp_count, rows, tokens),
        value_part.astype(jnp.bfloat16).reshape(dp_count // fast, fast, rows, value_columns),
        gain_part.reshape(dp_count, 1, rows),
    )
    own_output = lax.dynamic_slice_in_dim(
        new_rows.reshape(micro_count, 2, sequence_length, model_width),
        tensor_index * own_rows,
        own_rows,
        1,
    )
    return (own_output[None], value_share[None], mixed_share[None], gain_rows)


def solution(mesh):
    in_specs = (
        P("pipe", "dp", None, None, None),
        P("pipe", "dp", None, "tensor", None, None),
        P("pipe", None),
        P("pipe", None, "tensor"),
        P("pipe", "tensor", None),
        P("dp", "tensor", None, None),
        P("dp", None, None),
        P("dp", None),
        P("dp", None),
    )
    out_specs = (
        P("pipe", "dp", "tensor", None, None),
        P("pipe", "dp", "tensor"),
        P("pipe", "dp", "tensor"),
        P("pipe", "dp"),
    )
    return jax.shard_map(body, mesh=mesh, in_specs=in_specs, out_specs=out_specs, check_vma=False)
```
